256 devices in a mesh: gx: 8 (over z), gy: 32 (over x, y, core).
Axes of the slice: x: 4, y: 4, z: 8, core: 2. Of those that a mesh axis runs over, the one named last changes fastest.
Arguments:
- right_side: float32 [4096, 16384], P('gx', 'gy'), may hold values from -8 to 8
- drift_x: float32 [4096, 16384], P('gx', 'gy'), may hold values from -0.9 to 0.9
- drift_y: float32 [4096, 16384], P('gx', 'gy'), may hold values from -0.9 to 0.9
- sketch_rows: float32 [256, 4096], P(None, 'gx'), may hold values from -0.375 to 0.375
- sketch_cols: float32 [256, 16384], P(None, 'gy'), may hold values from -6 to 6
Outputs:
- solution: float32 [4096, 16384], P('gx', 'gy')
- residual: float32 [4096, 16384], P('gx', 'gy')
The draws below stay inside these ranges and needn't reach their ends.
All inputs are finite; a program needn't handle non-finite values.
Results may differ from the reference program's by a relative error of at most 0.0003.
Values sent between devices are 32-bit elements; how exact they have to be, the bound alone decides.
No kernel may reach another device: no remote copies, remote signals or barrier semaphores. Data moves between devices by JAX's collectives and lax.ppermute only.
A program may use at most 64 MiB of HBM per device.

```python
import jax
import jax.numpy as jnp
from jax import lax

K = 256
ITERS = 4
NX = 4096
NY = 16384


def block_scale(stream_key, shape, pieces, smallest, largest):
    loudness, own = 1.0, jax.random.fold_in(stream_key, 6)
    for axis_at, parts in pieces:
        draws = jnp.exp(jax.random.uniform(jax.random.fold_in(own, axis_at), (parts,), jnp.float32, smallest / len(pieces), largest / len(pieces)))
        loudness = loudness * jnp.repeat(draws, shape[axis_at] // parts).reshape([-1 if axis == axis_at else 1 for axis in range(len(shape))])
    return loudness


def noise(key, shape, scale, most, shards=(), kind=jnp.bfloat16):
    level = block_scale(key, shape, shards, -0.22, 0.18) if shards else 1.0
    values = jax.random.normal(key, shape, jnp.float32) * scale * level
    return jnp.minimum(jnp.maximum(values, -most), most).astype(kind)


def setup_inputs(seed: int = 0) -> dict:
    keys = jax.random.split(jax.random.key(seed), 6)
    right_side = noise(keys[0], (NX, NY), 1.0, 8.0, ((0, 8), (1, 32)), jnp.float32)
    drift_x = jnp.clip(jax.random.uniform(keys[1], (NX, NY), jnp.float32, -0.9, 0.9) * block_scale(keys[1], (NX, NY), ((0, 8), (1, 32)), -0.4, 0.0), -0.9, 0.9)
    drift_y = jnp.clip(jax.random.uniform(keys[2], (NX, NY), jnp.float32, -0.9, 0.9) * block_scale(keys[2], (NX, NY), ((0, 8), (1, 32)), -0.4, 0.0), -0.9, 0.9)
    sketch_rows = noise(keys[3], (K, NX), K ** -0.5, 0.375, ((1, 8),), jnp.float32)
    sketch_cols = noise(keys[4], (K, NY), 1.0, 6.0, ((1, 32),), jnp.float32)
    return dict(right_side=right_side, drift_x=drift_x, drift_y=drift_y, sketch_rows=sketch_rows, sketch_cols=sketch_cols)


shift_value = 0.05

def operate(field, drift_x, drift_y):
    padded = jnp.pad(field, 1)
    upper_cells = padded[:-2, 1:-1]
    lower_cells = padded[2:, 1:-1]
    left_cells = padded[1:-1, :-2]
    right_cells = padded[1:-1, 2:]
    return (4.0 + shift_value) * field - (1.0 + drift_x) * upper_cells - (1.0 - drift_x) * lower_cells - (1.0 + drift_y) * left_cells - (1.0 - drift_y) * right_cells

def sketch(field, sketch_rows, sketch_cols):
    product = jnp.dot(field, sketch_cols.T, precision=lax.Precision.HIGHEST)
    return jnp.einsum('ki,ik->k', sketch_rows, product, precision=lax.Precision.HIGHEST)

def solve_small(hessenberg, beta_norm):
    gram_matrix = jnp.dot(hessenberg.T, hessenberg, precision=lax.Precision.HIGHEST)
    target = beta_norm * hessenberg[0]
    factor = jnp.linalg.cholesky(gram_matrix)
    count = hessenberg.shape[1]
    forward = []
    for row in range(count):
        acc = target[row]
        for col in range(row):
            acc = acc - factor[row, col] * forward[col]
        forward.append(acc / factor[row, row])
    backward = [None] * count
    for row in reversed(range(count)):
        acc = forward[row]
        for col in range(row + 1, count):
            acc = acc - factor[col, row] * backward[col]
        backward[row] = acc / factor[row, row]
    return backward

def reference(right_side, drift_x, drift_y, sketch_rows, sketch_cols):
    first_sketch = sketch(right_side, sketch_rows, sketch_cols)
    beta_norm = jnp.sqrt(jnp.sum(first_sketch * first_sketch))
    basis_vectors = [right_side / beta_norm]
    sketched = [first_sketch / beta_norm]
    columns = []
    for column in range(ITERS):
        applied = operate(basis_vectors[column], drift_x, drift_y)
        sketch_image = sketch(applied, sketch_rows, sketch_cols)
        sketch_matrix = jnp.stack(sketched, axis=1)
        projection = jnp.dot(sketch_matrix.T, sketch_image, precision=lax.Precision.HIGHEST)
        remainder = applied
        for index_prev in range(column + 1):
            remainder = remainder - projection[index_prev] * basis_vectors[index_prev]
        remainder_sketch = sketch(remainder, sketch_rows, sketch_cols)
        new_norm = jnp.sqrt(jnp.sum(remainder_sketch * remainder_sketch))
        basis_vectors.append(remainder / new_norm)
        sketched.append(remainder_sketch / new_norm)
        entries = jnp.concatenate([projection, new_norm[None], jnp.zeros((ITERS - column - 1,), jnp.float32)])
        columns.append(entries)
    hessenberg = jnp.stack(columns, axis=1)
    coeffs = solve_small(hessenberg, beta_norm)
    solution = jnp.zeros_like(right_side)
    for column in range(ITERS):
        solution = solution + coeffs[column] * basis_vectors[column]
    residual = right_side - operate(solution, drift_x, drift_y)
    return (solution, residual)
```

```python
import functools

import jax
import jax.numpy as jnp
from jax import lax
from jax.experimental import pallas as pl
from jax.experimental.pallas import tpu as pltpu
from jax.sharding import Mesh
from jax.sharding import PartitionSpec as P

ITERS = 4
GY = ("x", "y", "c")
NEAR = ("z", "x")
FAR = ("y", "c")
F32 = jnp.float32
BF16 = jnp.bfloat16
DIAG = 4.0 + 0.05
LANES = 128
MIB = 1024 * 1024


def iota(shape, dim):
    return lax.broadcasted_iota(jnp.int32, shape, dim)


def vmem():
    return pl.BlockSpec(memory_space=pltpu.VMEM)


def params(limit=40):
    return pltpu.CompilerParams(vmem_limit_bytes=limit * MIB)


def rows_kernel(b0, x0, y0, b1, x1, y1, first, last):
    ones = jnp.ones((4, b0.shape[1]), F32)
    first[...] = jnp.concatenate([b0[0:4, :], x0[0:4, :], y0[0:4, :], ones], axis=0)
    last[...] = jnp.concatenate([b1[4:8, :], x1[4:8, :], y1[4:8, :], ones], axis=0)


def edge_rows(b, dx, dy):
    rows, width = b.shape
    low = pl.BlockSpec((8, width), lambda i: (0, 0))
    high = pl.BlockSpec((8, width), lambda i: (rows // 8 - 1, 0))
    out = pl.BlockSpec((16, width), lambda i: (0, 0))
    return pl.pallas_call(
        rows_kernel,
        grid=(1,),
        in_specs=[low] * 3 + [high] * 3,
        out_specs=[out] * 2,
        out_shape=[jax.ShapeDtypeStruct((16, width), F32)] * 2,
        name="edge_rows",
    )(b, dx, dy, b, dx, dy)


def columns_kernel(b0, x0, y0, b1, x1, y1, first, last):
    lane = iota(b0.shape, 1)
    one = jnp.ones(b0.shape, F32)
    packed = jnp.where(lane < 4, b0[...], pltpu.roll(x0[...], 4, 1))
    packed = jnp.where(lane < 8, packed, pltpu.roll(y0[...], 8, 1))
    packed = jnp.where(lane < 12, packed, one)
    first[...] = packed.T[0:16, :]
    packed = jnp.where(lane < 4, pltpu.roll(b1[...], 4, 1), pltpu.roll(x1[...], 8, 1))
    packed = jnp.where(lane < 8, packed, pltpu.roll(y1[...], 12, 1))
    packed = jnp.where(lane < 12, packed, one)
    last[...] = packed.T[0:16, :]


def edge_columns(b, dx, dy):
    rows, width = b.shape
    low = pl.BlockSpec((rows, LANES), lambda i: (0, 0))
    high = pl.BlockSpec((rows, LANES), lambda i: (0, width // LANES - 1))
    out = pl.BlockSpec((16, rows), lambda i: (0, 0))
    return pl.pallas_call(
        columns_kernel,
        grid=(1,),
        in_specs=[low] * 3 + [high] * 3,
        out_specs=[out] * 2,
        out_shape=[jax.ShapeDtypeStruct((16, rows), F32)] * 2,
        compiler_params=params(),
        name="edge_columns",
    )(b, dx, dy, b, dx, dy)


def split(value):
    high = value.astype(BF16)
    return high, (value - high.astype(F32)).astype(BF16)


def factors_kernel(cols, rows, right, rows_t):
    high, low = split(cols[...].T)
    n = high.shape[0]
    right[0:n, :] = high
    right[n : 2 * n, :] = high
    right[2 * n : 3 * n, :] = low
    rows_t[...] = rows[...].T


def factors(sketch_cols, sketch_rows):
    k, n = sketch_cols.shape
    m = sketch_rows.shape[1]
    return pl.pallas_call(
        factors_kernel,
        out_shape=[jax.ShapeDtypeStruct((3 * n, k), BF16), jax.ShapeDtypeStruct((m, k), F32)],
        in_specs=[vmem()] * 2,
        out_specs=[vmem()] * 2,
        compiler_params=params(),
        name="factors",
    )(sketch_cols, sketch_rows)


def neighbours(prev, cur, nxt):
    rows, width = cur.shape
    row = iota(cur.shape, 0)
    up = jnp.where(row == 0, prev[7:8, :], pltpu.roll(cur, 1, 0))
    down = jnp.where(row == rows - 1, nxt[0:1, :], pltpu.roll(cur, rows - 1, 0))
    left = pltpu.roll(cur, 1, 1)
    right = pltpu.roll(cur, width - 1, 1)
    return up, down, left, right


def krylov_kernel(
    copies, b, dx, dy, right, rows_t, top, bottom, from_left, from_right,
    t0, t1, t2, t3, t4, out, split_ref, side_dx, side_dy, side_one, tb_dx, tb_dy, tb_one, turn,
):
    rows, width = b.shape
    full = width + LANES
    lane = iota((rows, LANES), 1)
    inside = (lane < 4) | (lane >= LANES - 4)
    turn[...] = jnp.zeros_like(turn)
    for group in range(4):
        turn[8 * group : 8 * group + 4, :] = from_right[4 * group : 4 * group + 4, 0:rows]
        at = (8 * group - 4) % LANES
        turn[at : at + 4, :] = from_left[4 * group : 4 * group + 4, 0:rows]
    turned = turn[...].T
    zero = jnp.zeros((rows, LANES), F32)
    t0[0:rows + 16, width:full] = jnp.zeros((rows + 16, LANES), F32)
    t0[8 : rows + 8, width:full] = jnp.where(inside, turned, zero)
    side_dx[...] = jnp.where(inside, pltpu.roll(turned, LANES - 8, 1), zero)
    side_dy[...] = jnp.where(inside, pltpu.roll(turned, LANES - 16, 1), zero)
    side_one[...] = jnp.where(inside, pltpu.roll(turned, LANES - 24, 1), zero)
    t0[8 : rows + 8, 0:width] = b[...]
    lane = iota((4, LANES), 1)
    zero = jnp.zeros((4, LANES), F32)
    blank = jnp.zeros((4, full), F32)

    def strip(main, at, group):
        part = slice(4 * group, 4 * group + 4)
        corner = jnp.where(lane < 4, from_right[part, at : at + LANES], zero)
        corner = jnp.where(lane >= LANES - 4, from_left[part, at : at + LANES], corner)
        return jnp.concatenate([main[part, :], corner], axis=1)

    def above(group):
        return jnp.concatenate([blank, strip(top, rows, group)], axis=0)

    def below(group):
        return jnp.concatenate([strip(bottom, rows + LANES, group), blank], axis=0)

    t0[0:8, :] = above(0)
    t0[rows + 8 : rows + 16, :] = below(0)
    for ref, group in ((tb_dx, 1), (tb_dy, 2), (tb_one, 3)):
        ref[0:8, :] = above(group)
        ref[8:16, :] = below(group)

    fields = (t0, t1, t2, t3, t4)

    def advance(k, at, count, drift_x, drift_y, one):
        old = fields[k]
        cur = old[pl.ds(at, count), :]
        prev = old[pl.ds(max(at - 8, 0) if isinstance(at, int) else pl.multiple_of(at - 8, 8), 8), :]
        after = min(at + count, rows + 8) if isinstance(at, int) else pl.multiple_of(at + count, 8)
        nxt = old[pl.ds(after, 8), :]
        up, down, left, right_ = neighbours(prev, cur, nxt)
        cross = up + down + (left + right_)
        if one is not None:
            cross = jnp.concatenate([cross[:, :width], cross[:, width:] * one], axis=1) if one.shape[1] == LANES else cross * one
        new = cross + drift_x * (up - down) + drift_y * (left - right_)
        if k == 0:
            return 0.25 * new
        return 0.5 * new - fields[k - 1][pl.ds(at, count), :]

    def keep(at, value):
        high, low = split(value)
        split_ref[pl.ds(at, 16), 0:width] = high
        split_ref[pl.ds(at, 16), width : 2 * width] = low
        split_ref[pl.ds(at, 16), 2 * width : 3 * width] = high

    total = []

    def sketch():
        product = jnp.dot(split_ref[...], right[...], preferred_element_type=F32)
        total.append(jnp.sum(product * rows_t[...], axis=0, keepdims=True))

    def first(i, carry):
        at = pl.multiple_of(i * 16, 16)
        keep(at, b[pl.ds(at, 16), :])
        return carry

    lax.fori_loop(0, rows // 16, first, 0)
    sketch()
    for k in range(ITERS):
        new = fields[k + 1]
        if k < ITERS - 1:
            for at in (0, rows + 8):
                tb = slice(0, 8) if at == 0 else slice(8, 16)
                new[at : at + 8, :] = advance(k, at, 8, tb_dx[tb, :], tb_dy[tb, :], tb_one[tb, :])

        def block(i, carry, k=k, new=new):
            at = pl.multiple_of(i * 16, 16)
            here = pl.ds(at, 16)
            drift_x = jnp.concatenate([dx[here, :], side_dx[here, :]], axis=1)
            drift_y = jnp.concatenate([dy[here, :], side_dy[here, :]], axis=1)
            value = advance(k, pl.multiple_of(at + 8, 8), 16, drift_x, drift_y, side_one[here, :])
            if k < ITERS - 1:
                new[pl.ds(pl.multiple_of(at + 8, 8), 16), :] = value
            else:
                new[here, :] = value[:, :width]
            keep(at, value[:, :width])
            return carry

        lax.fori_loop(0, rows // 16, block, 0, unroll=2)
        sketch()
    whole = jnp.concatenate(total, axis=1)
    for i in range(copies):
        out[i] = whole


def krylov(b, dx, dy, right, rows_t, top, bottom, from_left, from_right, copies):
    rows, width = b.shape
    full = width + LANES
    k = rows_t.shape[1]
    padded = jax.ShapeDtypeStruct((rows + 16, full), F32)
    return pl.pallas_call(
        functools.partial(krylov_kernel, copies),
        out_shape=[padded] * 4
        + [jax.ShapeDtypeStruct((rows, width), F32), jax.ShapeDtypeStruct((copies, 1, (ITERS + 1) * k), F32)],
        in_specs=[vmem()] * 9,
        out_specs=[vmem()] * 6,
        scratch_shapes=[
            pltpu.VMEM((rows, 3 * width), BF16),
            pltpu.VMEM((rows, LANES), F32),
            pltpu.VMEM((rows, LANES), F32),
            pltpu.VMEM((rows, LANES), F32),
            pltpu.VMEM((16, full), F32),
            pltpu.VMEM((16, full), F32),
            pltpu.VMEM((16, full), F32),
            pltpu.VMEM((LANES, rows), F32),
        ],
        compiler_params=params(),
        name="krylov",
    )(b, dx, dy, right, rows_t, top, bottom, from_left, from_right)


def combine_kernel(parts, t0, t1, t2, t3, t4, sol, res, coef):
    @pl.when(pl.program_id(0) == 0)
    def _():
        k = parts.shape[2] // (ITERS + 1)
        whole = parts[0]
        for i in range(1, parts.shape[0]):
            whole = whole + parts[i]
        s = [whole[:, i * k : (i + 1) * k] for i in range(ITERS + 1)]
        images = [DIAG * s[0] - 4.0 * s[1]]
        for i in range(1, ITERS):
            images.append(DIAG * s[i] - 2.0 * (s[i + 1] + s[i - 1]))
        left = jnp.concatenate(images + [s[0]] + [jnp.zeros_like(s[0])] * (7 - ITERS), axis=0)
        ratios = []
        row = iota((8, 1), 0)
        for j in range(ITERS):
            q = left[j : j + 1, :]
            dots = jnp.sum(left * q, axis=1, keepdims=True)
            ratio = dots / dots[j : j + 1, :]
            ratios.append(ratio)
            left = left - jnp.where(row > j, ratio, 0.0) * q
        c = [None] * ITERS
        for j in reversed(range(ITERS)):
            value = ratios[j][ITERS : ITERS + 1, :]
            for i in range(j + 1, ITERS):
                value = value - ratios[j][i : i + 1, :] * c[i]
            c[j] = value
        d = [
            1.0 - DIAG * c[0] + 2.0 * c[1],
            4.0 * c[0] - DIAG * c[1] + 2.0 * c[2],
            2.0 * c[1] - DIAG * c[2] + 2.0 * c[3],
            2.0 * c[2] - DIAG * c[3],
            2.0 * c[3],
        ]
        for i, value in enumerate(c + d):
            coef[i] = jnp.broadcast_to(value, coef.shape[1:])

    rows, width = sol.shape

    def block(i, carry):
        at = pl.multiple_of(i * 8, 8)
        start = pl.multiple_of(pl.program_id(0) * rows + at, 8)
        shifted = pl.ds(pl.multiple_of(start + 8, 8), 8)
        for j in range(width // LANES):
            lanes = slice(j * LANES, (j + 1) * LANES)
            t = [ref[shifted, lanes] for ref in (t0, t1, t2, t3)] + [t4[pl.ds(start, 8), lanes]]
            first = coef[0] * t[0] + coef[1] * t[1]
            second = coef[4] * t[0] + coef[5] * t[1]
            sol[pl.ds(at, 8), lanes] = first + (coef[2] * t[2] + coef[3] * t[3])
            res[pl.ds(at, 8), lanes] = second + (coef[6] * t[2] + coef[7] * t[3]) + coef[8] * t[4]
        return carry

    lax.fori_loop(0, rows // 8, block, 0, unroll=2)


def combine(parts, fields):
    rows, width = fields[-1].shape
    steps = 4
    out = pl.BlockSpec((rows // steps, width), lambda i: (i, 0))
    return pl.pallas_call(
        combine_kernel,
        grid=(steps,),
        in_specs=[vmem()] * 6,
        out_specs=[out] * 2,
        out_shape=[jax.ShapeDtypeStruct((rows, width), F32)] * 2,
        scratch_shapes=[pltpu.VMEM((2 * ITERS + 1, 8, LANES), F32)],
        compiler_params=params(),
        name="combine",
    )(parts, *fields)


def shift(value, axis, step):
    size = lax.axis_size(axis)
    pairs = [(i, i + step) for i in range(size) if 0 <= i + step < size]
    return lax.ppermute(value, axis, pairs)


def to_all(copies, axis):
    return lax.all_to_all(copies, axis, split_axis=0, concat_axis=0, tiled=True)


def body(right_side, drift_x, drift_y, sketch_rows, sketch_cols):
    first, last = edge_rows(right_side, drift_x, drift_y)
    top, bottom = shift(last, "z", 1), shift(first, "z", -1)
    first_columns, last_columns = edge_columns(right_side, drift_x, drift_y)
    right, rows_t = factors(sketch_cols, sketch_rows)
    to_left = jnp.concatenate([first_columns, top[:, :LANES], bottom[:, :LANES]], axis=1)
    to_right = jnp.concatenate([last_columns, top[:, -LANES:], bottom[:, -LANES:]], axis=1)
    from_left, from_right = shift(to_right, GY, 1), shift(to_left, GY, -1)
    near, far = lax.axis_size(NEAR), lax.axis_size(FAR)
    *fields, partial = krylov(
        right_side, drift_x, drift_y, right, rows_t, top, bottom, from_left, from_right, near
    )
    summed = jnp.sum(to_all(partial, NEAR), axis=0, keepdims=True)
    parts = to_all(jnp.broadcast_to(summed, (far, *summed.shape[1:])), FAR)
    return tuple(combine(parts, fields))


def solution(mesh):
    split_mesh = Mesh(mesh.devices.reshape(mesh.shape["gx"], 4, 4, 2), ("z", *GY))
    in_specs = (P("z", GY), P("z", GY), P("z", GY), P(None, "z"), P(None, GY))
    out_specs = (P("z", GY), P("z", GY))
    return jax.shard_map(body, mesh=split_mesh, in_specs=in_specs, out_specs=out_specs, check_vma=False)
```
